128 devices in a mesh: row: 8 (over x_lo, z), col: 16 (over y, x_hi, core).
Axes of the slice: x: 4 (x_hi: 2, x_lo: 2; x = x_hi * 2 + x_lo), y: 4, z: 4, core: 2. Of those that a mesh axis runs over, the one named last changes fastest.
Arguments:
- q_base: bfloat16 [8192, 8192], P('row', 'col'), may hold values from -600 to 600
- q_down: bfloat16 [64, 8192], P(None, 'col'), may hold values from -1.1953125 to 1.1953125
- q_up: bfloat16 [8192, 64], P('row'), may hold values from -1.1953125 to 1.1953125
- q_magnitude: float32 [8192], P('row'), may hold values from 40 to 200
- k_base: bfloat16 [1024, 8192], P('row', 'col'), may hold values from -600 to 600
- k_down: bfloat16 [64, 8192], P(None, 'col'), may hold values from -1.1953125 to 1.1953125
- k_up: bfloat16 [1024, 64], P('row'), may hold values from -1.1953125 to 1.1953125
- k_magnitude: float32 [1024], P('row'), may hold values from 40 to 200
- v_base: bfloat16 [1024, 8192], P('row', 'col'), may hold values from -600 to 600
- v_down: bfloat16 [64, 8192], P(None, 'col'), may hold values from -1.1953125 to 1.1953125
- v_up: bfloat16 [1024, 64], P('row'), may hold values from -1.1953125 to 1.1953125
- v_magnitude: float32 [1024], P('row'), may hold values from 40 to 200
- o_base: bfloat16 [8192, 8192], P('row', 'col'), may hold values from -600 to 600
- o_down: bfloat16 [64, 8192], P(None, 'col'), may hold values from -1.1953125 to 1.1953125
- o_up: bfloat16 [8192, 64], P('row'), may hold values from -1.1953125 to 1.1953125
- o_magnitude: float32 [8192], P('row'), may hold values from 40 to 200
- gate_base: bfloat16 [29568, 8192], P('row', 'col'), may hold values from -600 to 600
- gate_down: bfloat16 [64, 8192], P(None, 'col'), may hold values from -1.1953125 to 1.1953125
- gate_up: bfloat16 [29568, 64], P('row'), may hold values from -1.1953125 to 1.1953125
- gate_magnitude: float32 [29568], P('row'), may hold values from 40 to 200
- lift_base: bfloat16 [29568, 8192], P('row', 'col'), may hold values from -600 to 600
- lift_down: bfloat16 [64, 8192], P(None, 'col'), may hold values from -1.1953125 to 1.1953125
- lift_up: bfloat16 [29568, 64], P('row'), may hold values from -1.1953125 to 1.1953125
- lift_magnitude: float32 [29568], P('row'), may hold values from 40 to 200
Outputs:
- q_merged: bfloat16 [8192, 8192], P(('row', 'col'))
- k_merged: bfloat16 [1024, 8192], P(('row', 'col'))
- v_merged: bfloat16 [1024, 8192], P(('row', 'col'))
- o_merged: bfloat16 [8192, 8192], P(None, ('col', 'row'))
- gate_merged: bfloat16 [29568, 8192], P(('row', 'col'))
- lift_merged: bfloat16 [29568, 8192], P(('row', 'col'))
The draws below stay inside these ranges and needn't reach their ends.
All inputs are finite; a program needn't handle non-finite values.
Results may differ from the reference program's by a relative error of at most 0.001.
Values may be sent and summed in bfloat16 or wider, within the bound.
A program may use at most 128 MiB of HBM per device.

```python
import math
import jax
import jax.numpy as jnp
from jax import lax

D = 8192
FF = 29568
RANK = 64
KVD = 1024


def base_draw(key, height, breadth, salt):
    key = jax.random.fold_in(key, salt)
    first = jax.random.fold_in(key, 0)
    ramp = jnp.exp(math.log(3.0) * jnp.arange(breadth, dtype=jnp.float32) / (breadth - 1))
    values = jnp.clip(jax.random.normal(first, (height, breadth), jnp.float32), -6.0, 6.0) * ramp[None, :]
    return values.astype(jnp.bfloat16)


def draw_q_base(key, part):
    return base_draw(key, D, D, 11)


def draw_k_base(key, part):
    return base_draw(key, KVD, D, 12)


def draw_v_base(key, part):
    return base_draw(key, KVD, D, 13)


def draw_o_base(key, part):
    return base_draw(key, D, D, 14)


def draw_gate_base(key, part):
    return base_draw(key, FF, D, 15)


def draw_lift_base(key, part):
    return base_draw(key, FF, D, 16)


def block_levels(stream_key, extent, cuts, low, top_value):
    factor_of = 1.0
    for axis_at, shards_of in cuts:
        heights = jax.random.uniform(jax.random.fold_in(jax.random.fold_in(stream_key, 6), axis_at), (shards_of,), jnp.float32, low / len(cuts), top_value / len(cuts))
        factor_of = factor_of * jnp.repeat(jnp.exp(heights), extent[axis_at] // shards_of).reshape((-1,) + (1,) * (len(extent) - 1 - axis_at))
    return factor_of


def gaussian(rng, shape, spread, most, pieces=(), kind=jnp.bfloat16):
    array = spread * jax.random.normal(rng, shape, jnp.float32)
    if pieces:
        array = array * block_levels(rng, shape, pieces, -0.22, 0.18)
    return jnp.clip(array, -most, most).astype(kind)


def setup_inputs(seed: int = 0) -> dict:
    key_of = jax.random.split(jax.random.key(seed), 25)
    return {
        "q_base": draw_q_base(jax.random.fold_in(key_of[24], 71), 0),
        "q_down": gaussian(key_of[1], (RANK, D), 0.2, 1.1953125, ((1, 16),)),
        "q_up": gaussian(key_of[2], (D, RANK), 0.2, 1.1953125, ((0, 8),)),
        "q_magnitude": jnp.clip(jnp.exp(math.log(200.0) - 1.609438 * jax.random.uniform(key_of[3], (D,), jnp.float32) ** block_levels(key_of[3], (D,), ((0, 8),), -0.2, 0.2)), 40.0, 200.0),
        "k_base": draw_k_base(jax.random.fold_in(key_of[24], 71), 0),
        "k_down": gaussian(key_of[5], (RANK, D), 0.2, 1.1953125, ((1, 16),)),
        "k_up": gaussian(key_of[6], (KVD, RANK), 0.2, 1.1953125, ((0, 8),)),
        "k_magnitude": jnp.clip(jnp.exp(math.log(200.0) - 1.609438 * jax.random.uniform(key_of[7], (KVD,), jnp.float32) ** block_levels(key_of[7], (KVD,), ((0, 8),), -0.2, 0.2)), 40.0, 200.0),
        "v_base": draw_v_base(jax.random.fold_in(key_of[24], 71), 0),
        "v_down": gaussian(key_of[9], (RANK, D), 0.2, 1.1953125, ((1, 16),)),
        "v_up": gaussian(key_of[10], (KVD, RANK), 0.2, 1.1953125, ((0, 8),)),
        "v_magnitude": jnp.clip(jnp.exp(math.log(200.0) - 1.609438 * jax.random.uniform(key_of[11], (KVD,), jnp.float32) ** block_levels(key_of[11], (KVD,), ((0, 8),), -0.2, 0.2)), 40.0, 200.0),
        "o_base": draw_o_base(jax.random.fold_in(key_of[24], 71), 0),
        "o_down": gaussian(key_of[13], (RANK, D), 0.2, 1.1953125, ((1, 16),)),
        "o_up": gaussian(key_of[14], (D, RANK), 0.2, 1.1953125, ((0, 8),)),
        "o_magnitude": jnp.clip(jnp.exp(math.log(200.0) - 1.609438 * jax.random.uniform(key_of[15], (D,), jnp.float32) ** block_levels(key_of[15], (D,), ((0, 8),), -0.2, 0.2)), 40.0, 200.0),
        "gate_base": draw_gate_base(jax.random.fold_in(key_of[24], 71), 0),
        "gate_down": gaussian(key_of[17], (RANK, D), 0.2, 1.1953125, ((1, 16),)),
        "gate_up": gaussian(key_of[18], (FF, RANK), 0.2, 1.1953125, ((0, 8),)),
        "gate_magnitude": jnp.clip(jnp.exp(math.log(200.0) - 1.609438 * jax.random.uniform(key_of[19], (FF,), jnp.float32) ** block_levels(key_of[19], (FF,), ((0, 8),), -0.2, 0.2)), 40.0, 200.0),
        "lift_base": draw_lift_base(jax.random.fold_in(key_of[24], 71), 0),
        "lift_down": gaussian(key_of[21], (RANK, D), 0.2, 1.1953125, ((1, 16),)),
        "lift_up": gaussian(key_of[22], (FF, RANK), 0.2, 1.1953125, ((0, 8),)),
        "lift_magnitude": jnp.clip(jnp.exp(math.log(200.0) - 1.609438 * jax.random.uniform(key_of[23], (FF,), jnp.float32) ** block_levels(key_of[23], (FF,), ((0, 8),), -0.2, 0.2)), 40.0, 200.0),
    }


eps = 1e-06

def merge_one(base, down, up, magnitude):
    direction = base.astype(jnp.float32) + jnp.dot(up, down, preferred_element_type=jnp.float32)
    total = lax.optimization_barrier(jnp.sum(direction * direction, axis=1))
    factor = magnitude * lax.rsqrt(total + eps)
    return (direction * factor[:, None]).astype(jnp.bfloat16)

def reference(q_base, q_down, q_up, q_magnitude, k_base, k_down, k_up, k_magnitude, v_base, v_down, v_up, v_magnitude, o_base, o_down, o_up, o_magnitude, gate_base, gate_down, gate_up, gate_magnitude, lift_base, lift_down, lift_up, lift_magnitude):
    return (merge_one(q_base, q_down, q_up, q_magnitude), merge_one(k_base, k_down, k_up, k_magnitude), merge_one(v_base, v_down, v_up, v_magnitude), merge_one(o_base, o_down, o_up, o_magnitude), merge_one(gate_base, gate_down, gate_up, gate_magnitude), merge_one(lift_base, lift_down, lift_up, lift_magnitude))
```

```python
import jax
import jax.numpy as jnp
from jax import lax
from jax.experimental import pallas as pl
from jax.experimental.pallas import tpu as pltpu
from jax.sharding import PartitionSpec as P

MESH = pl.DeviceIdType.MESH
NAMES = ("q", "k", "v", "o", "gate", "lift")
ROW_SPLIT = ("k", "v", "q", "gate", "lift")
eps = 1e-06
LANES = 128


def up_to(value, unit):
    return -(-value // unit) * unit


class Plan:
    def __init__(self, mesh, bases, rank):
        self.rows_n = mesh.shape["row"]
        self.cols_n = mesh.shape["col"]
        self.rank = rank
        self.height = {p: b.shape[0] for p, b in bases.items()}
        self.width = bases["q"].shape[1]
        self.tiles = {p: -(-h // LANES) for p, h in self.height.items()}
        self.block = {p: self.height[p] // self.cols_n for p in ROW_SPLIT}
        self.held = {p: up_to(self.block[p], 8) for p in ROW_SPLIT}
        self.first = {}
        count = 0
        for p in ("o", "gate", "lift"):
            self.first[p] = count
            count += self.tiles[p]
        self.share = -(-count // self.cols_n)
        assert self.share <= 8


def column_sums(square):
    folded = square[:, :LANES]
    for at in range(LANES, square.shape[1], LANES):
        folded = folded + square[:, at : at + LANES]
    return jnp.sum(folded.T, axis=0, keepdims=True)


def kernel(plan, *refs):
    cols_n, rows_n = plan.cols_n, plan.rows_n
    width, rank = plan.width, plan.rank
    it = iter(refs)
    base = {p: None for p in NAMES}
    down, up, mag = dict(base), dict(base), dict(base)
    for p in NAMES:
        base[p], down[p], up[p], mag[p] = next(it), next(it), next(it), next(it)
    out = {p: next(it) for p in NAMES}
    stage, downs, ups, mags = {}, {}, {}, {}
    for p in NAMES:
        stage[p], downs[p], ups[p], mags[p] = next(it), next(it), next(it), next(it)
    wide = {p: next(it) for p in NAMES}
    send = {p: next(it) for p in NAMES}
    scale = next(it)
    spare = next(it)
    sums_kv, sums_q, parts, owned, totals = (next(it) for _ in range(5))
    load_sem, own_sem, send_sem, recv_sem = (next(it) for _ in range(4))

    me = lax.axis_index("col")
    my_row = lax.axis_index("row")

    order = ("k", "v", "q", "o", "gate", "lift")
    loads = {}
    for i, p in enumerate(order):
        loads[p] = [
            pltpu.make_async_copy(src[p], dst[p], load_sem.at[4 * i + j])
            for j, (src, dst) in enumerate(((base, stage), (down, downs), (up, ups), (mag, mags)))
        ]
        for copy in loads[p]:
            copy.start()

    barrier = pltpu.get_barrier_semaphore()
    for s in range(1, cols_n):
        pl.semaphore_signal(
            barrier, inc=1, device_id={"col": lax.rem(me + s, cols_n)}, device_id_type=MESH
        )
    for s in range(1, rows_n):
        pl.semaphore_signal(
            barrier, inc=1, device_id={"row": lax.rem(my_row + s, rows_n)}, device_id_type=MESH
        )

    def col_copy(kind, s, src, dst):
        return pltpu.make_async_remote_copy(
            src_ref=src,
            dst_ref=dst,
            send_sem=send_sem.at[kind, s],
            recv_sem=recv_sem.at[kind, s],
            device_id={"col": lax.rem(me + s, cols_n)},
            device_id_type=MESH,
        )

    def each(fn):
        def step(s, carry):
            fn(s)
            return carry

        lax.fori_loop(1, cols_n, step, 0)

    def product(p, at, size):
        return lax.dot_general(
            ups[p][:, pl.ds(at, size)],
            downs[p][...],
            (((0,), (0,)), ((), ())),
            preferred_element_type=jnp.float32,
        )

    def direction(p, at, size):
        return stage[p][pl.ds(at, size), :].astype(jnp.float32) + product(p, at, size)

    def first_pass(p, put):
        height = plan.height[p]
        full = height // LANES

        def tile(t, carry):
            at = pl.multiple_of(t * LANES, LANES)
            d = direction(p, at, LANES)
            wide[p][pl.ds(at, LANES), :] = d
            put(t, column_sums(d * d))
            return carry

        lax.fori_loop(0, full, tile, 0)
        rest = height - full * LANES
        if rest:
            at = full * LANES
            d = direction(p, at, rest)
            wide[p][pl.ds(at, rest), :] = d
            fill = jnp.zeros((LANES - rest, width), jnp.float32)
            wide[p][pl.ds(at + rest, LANES - rest), :] = fill
            square = jnp.concatenate([d * d, fill], axis=0)
            put(full, column_sums(square))

    def first_pass_o(put):
        def tile(t, carry):
            at = pl.multiple_of(t * LANES, LANES)
            d = direction("o", at, LANES).T
            wide["o"][:, pl.ds(at, LANES)] = d
            put(t, jnp.sum(d * d, axis=0, keepdims=True))
            return carry

        lax.fori_loop(0, plan.tiles["o"], tile, 0)

    def magnitudes(p, t):
        full = plan.height[p] // LANES
        if isinstance(t, int) and t == full:
            rest = plan.height[p] - full * LANES
            spare[...] = jnp.zeros_like(spare)
            spare[0:1, 0:rest] = mags[p][:, full * LANES :]
            return spare[0:1, :]
        return mags[p][:, pl.ds(pl.multiple_of(t * LANES, LANES), LANES)]

    def factors(p, t, total):
        return magnitudes(p, t) * lax.rsqrt(total + eps)

    def fill_scale(p, total_of):
        def one(t):
            row = factors(p, t, total_of(t))
            at = t * LANES if isinstance(t, int) else pl.multiple_of(t * LANES, LANES)
            scale[pl.ds(at, LANES), :] = jnp.broadcast_to(row, (LANES, LANES)).T

        full = plan.height[p] // LANES

        def tile(t, carry):
            one(t)
            return carry

        lax.fori_loop(0, full, tile, 0)
        if plan.tiles[p] > full:
            one(full)

    def merged(p, at, size):
        factor = scale[pl.ds(at, size), :]
        return jnp.concatenate(
            [
                (wide[p][pl.ds(at, size), c : c + LANES] * factor).astype(jnp.bfloat16)
                for c in range(0, width, LANES)
            ],
            axis=1,
        )

    def block_copy(p, kind, s):
        target = lax.rem(me + s, cols_n)
        return col_copy(
            kind,
            s,
            send[p].at[target],
            out[p].at[:, pl.ds(pl.multiple_of(me * width, width), width)],
        )

    own = []

    def own_block(p, src, dst):
        copy = pltpu.make_async_copy(src, dst, own_sem.at[NAMES.index(p)])
        copy.start()
        own.append(copy)

    def own_rows(p):
        own_block(
            p, send[p].at[me], out[p].at[:, pl.ds(pl.multiple_of(me * width, width), width)]
        )

    KIND = {p: i for i, p in enumerate(ROW_SPLIT)}
    KV, Q, RS, AG = (len(ROW_SPLIT) + i for i in range(4))

    def tally(kind, buffer, wait_copy):
        each(lambda s: wait_copy(s).wait_recv())
        total = buffer[0]
        for c in range(1, cols_n):
            total = total + buffer[c]
        return total

    for p in ("k", "v"):
        for copy in loads[p]:
            copy.wait()
    sums_kv[me] = jnp.zeros(sums_kv.shape[1:], jnp.float32)
    for i, p in enumerate(("k", "v")):

        def put(t, sums, i=i):
            sums_kv[pl.ds(me, 1), i, :] = sums

        first_pass(p, put)

    pl.semaphore_wait(barrier, cols_n + rows_n - 2)

    def kv_copy(s):
        return col_copy(KV, s, sums_kv.at[me], sums_kv.at[me])

    each(lambda s: kv_copy(s).start())

    for copy in loads["q"]:
        copy.wait()

    def put_q(t, sums):
        sums_q[pl.ds(me, 1), pl.ds(t, 1), :] = sums.reshape(1, 1, LANES)

    first_pass("q", put_q)

    def q_copy(s):
        return col_copy(Q, s, sums_q.at[me], sums_q.at[me])

    each(lambda s: q_copy(s).start())

    parts[...] = jnp.zeros_like(parts)

    def put_later(p):
        def put(t, sums):
            slot = plan.first[p] + t
            owner, at = slot // plan.share, slot % plan.share
            parts[pl.ds(owner, 1), pl.ds(at, 1), :] = sums.reshape(1, 1, LANES)

        return put

    for copy in loads["o"]:
        copy.wait()
    first_pass_o(put_later("o"))

    total = tally(KV, sums_kv, kv_copy)
    for i, p in enumerate(("k", "v")):
        fill_scale(p, lambda t, i=i: total[i : i + 1, :])
        block = plan.block[p]
        for c in range(cols_n):
            send[p][c] = merged(p, c * block, block)
        each(lambda s, p=p: block_copy(p, KIND[p], s).start())
        own_rows(p)

    totals_q = tally(Q, sums_q, q_copy)
    spare[...] = totals_q
    fill_scale("q", lambda t: spare[pl.ds(t, 1), :])
    block = plan.block["q"]

    def q_block(c, carry):
        send["q"][c] = merged("q", pl.multiple_of(c * block, block), block)
        return carry

    lax.fori_loop(0, cols_n, q_block, 0)
    each(lambda s: block_copy("q", KIND["q"], s).start())
    own_rows("q")

    for p in ("gate", "lift"):
        for copy in loads[p]:
            copy.wait()
        first_pass(p, put_later(p))

    def rs_copy(s):
        target = lax.rem(me + s, cols_n)
        return col_copy(RS, s, parts.at[target], owned.at[me])

    each(lambda s: rs_copy(s).start())
    owned[me] = parts[me]
    totals[me] = tally(RS, owned, rs_copy)

    def ag_copy(s):
        return col_copy(AG, s, totals.at[me], totals.at[me])

    each(lambda s: ag_copy(s).start())
    each(lambda s: ag_copy(s).wait_recv())

    def later_total(p):
        def of(t):
            slot = plan.first[p] + t
            owner, at = slot // plan.share, slot % plan.share
            return totals[pl.ds(owner, 1), pl.ds(at, 1), :].reshape(1, LANES)

        return of

    total_of_o = later_total("o")

    def o_tile(t, carry):
        at = pl.multiple_of(t * LANES, LANES)
        factor = factors("o", t, total_of_o(t))
        send["o"][:, pl.ds(at, LANES)] = (wide["o"][:, pl.ds(at, LANES)] * factor).astype(
            jnp.bfloat16
        )
        return carry

    lax.fori_loop(0, plan.tiles["o"], o_tile, 0)
    depth = width // rows_n
    height = plan.height["o"]
    O = AG + 1
    o_place = out["o"].at[:, pl.ds(pl.multiple_of(my_row * height, height), height)]

    def o_copy(s):
        target = lax.rem(my_row + s, rows_n)
        return pltpu.make_async_remote_copy(
            src_ref=send["o"].at[pl.ds(pl.multiple_of(target * depth, depth), depth), :],
            dst_ref=o_place,
            send_sem=send_sem.at[O, s],
            recv_sem=recv_sem.at[O, s],
            device_id={"row": target},
            device_id_type=MESH,
        )

    for s in range(1, rows_n):
        o_copy(s).start()
    own_block("o", send["o"].at[pl.ds(pl.multiple_of(my_row * depth, depth), depth), :], o_place)

    for p in ("gate", "lift"):
        fill_scale(p, later_total(p))
        block, held = plan.block[p], plan.held[p]
        window = up_to(block + 15, 128)
        ahead = lax.broadcasted_iota(jnp.int32, (held, window), 1) - lax.broadcasted_iota(
            jnp.int32, (held, window), 0
        )

        def make(target, p=p, block=block, window=window, ahead=ahead):
            start = target * block
            at = pl.multiple_of(start // 16 * 16, 16)
            pick = jnp.where(ahead == start - at, 1.0, 0.0).astype(jnp.bfloat16)
            rows = merged(p, at, window)
            send[p][target] = jnp.dot(pick, rows, preferred_element_type=jnp.float32).astype(
                jnp.bfloat16
            )

        def go(s, p=p, make=make):
            make(lax.rem(me + s, cols_n))
            block_copy(p, KIND[p], s).start()

        each(go)
        make(me)
        own_rows(p)

    each(lambda s: kv_copy(s).wait_send())
    each(lambda s: q_copy(s).wait_send())
    each(lambda s: rs_copy(s).wait_send())
    each(lambda s: ag_copy(s).wait_send())
    for p in ROW_SPLIT:
        each(lambda s, p=p: block_copy(p, KIND[p], s).wait())
    for s in range(1, rows_n):
        o_copy(s).wait()
    for copy in own:
        copy.wait()


def solution(mesh):
    def on_device(*args):
        bases = {p: args[4 * i] for i, p in enumerate(NAMES)}
        rank = args[1].shape[0]
        plan = Plan(mesh, bases, rank)
        width, cols_n = plan.width, plan.cols_n
        bf16, f32 = jnp.bfloat16, jnp.float32
        operands, scratch = [], []
        for i, p in enumerate(NAMES):
            base, down, up, magnitude = args[4 * i : 4 * i + 4]
            operands += [base, down, up.T, magnitude.reshape(1, -1)]
            scratch += [
                pltpu.VMEM(base.shape, bf16),
                pltpu.VMEM(down.shape, bf16),
                pltpu.VMEM((rank, base.shape[0]), bf16),
                pltpu.VMEM((1, base.shape[0]), f32),
            ]
        shapes = []
        for p in NAMES:
            if p == "o":
                shapes.append((width // plan.rows_n, plan.height[p] * plan.rows_n))
                scratch.append(pltpu.VMEM((width, plan.height[p]), f32))
            else:
                shapes.append((plan.held[p], width * cols_n))
                scratch.append(pltpu.VMEM((plan.tiles[p] * LANES, width), f32))
        for p in NAMES:
            if p == "o":
                scratch.append(pltpu.VMEM((width, plan.height[p]), bf16))
            else:
                scratch.append(pltpu.VMEM((cols_n, plan.held[p], width), bf16))
        scratch.append(pltpu.VMEM((max(plan.tiles.values()) * LANES, LANES), f32))
        scratch.append(pltpu.VMEM((8, LANES), f32))
        scratch += [pltpu.VMEM((cols_n, 8, LANES), f32)] * 5
        scratch += [
            pltpu.SemaphoreType.DMA((24,)),
            pltpu.SemaphoreType.DMA((6,)),
            pltpu.SemaphoreType.DMA((10, cols_n)),
            pltpu.SemaphoreType.DMA((10, cols_n)),
        ]
        got = pl.pallas_call(
            lambda *refs: kernel(plan, *refs),
            out_shape=[jax.ShapeDtypeStruct(s, bf16) for s in shapes],
            in_specs=[pl.BlockSpec(memory_space=pl.ANY)] * len(operands),
            out_specs=[pl.BlockSpec(memory_space=pl.ANY)] * len(shapes),
            scratch_shapes=scratch,
            name="merge",
            compiler_params=pltpu.CompilerParams(
                collective_id=0, has_side_effects=True, vmem_limit_bytes=62 * 1024 * 1024
            ),
        )(*operands)
        outs = []
        for p, o in zip(NAMES, got):
            outs.append(o.T if p == "o" else o[: plan.block[p]])
        return tuple(outs)

    specs = []
    for p in NAMES:
        specs += [P("row", "col"), P(None, "col"), P("row", None), P("row")]
    by_row = P(("row", "col"), None)
    return jax.shard_map(
        on_device,
        mesh=mesh,
        in_specs=tuple(specs),
        out_specs=(by_row, by_row, by_row, P(None, ("col", "row")), by_row, by_row),
        check_vma=False,
    )
```

```python
import jax
import jax.numpy as jnp
from jax import lax
from jax.experimental import pallas as pl
from jax.experimental.pallas import tpu as pltpu
from jax.sharding import PartitionSpec as P

MESH = pl.DeviceIdType.MESH
NAMES = ("q", "k", "v", "o", "gate", "lift")
ROW_SPLIT = ("k", "v", "q", "gate", "lift")
LATE = {"first": ("gate", "o"), "second": ("lift",)}
UNROLL = 4
eps = 1e-06
LANES = 128


def up_to(value, unit):
    return -(-value // unit) * unit


class Plan:
    def __init__(self, mesh, bases, rank):
        self.rows_n = mesh.shape["row"]
        self.cols_n = mesh.shape["col"]
        self.rank = rank
        self.height = {p: b.shape[0] for p, b in bases.items()}
        self.width = bases["q"].shape[1]
        self.tiles = {p: -(-h // LANES) for p, h in self.height.items()}
        self.block = {p: self.height[p] // self.cols_n for p in ROW_SPLIT}
        self.held = {p: up_to(self.block[p], 8) for p in ROW_SPLIT}
        self.begin, self.share = {}, {}
        for group, members in LATE.items():
            count = 0
            for p in members:
                self.begin[p] = (group, count)
                count += self.tiles[p]
            self.share[group] = -(-count // self.cols_n)
        self.early = {"k": 0, "v": self.tiles["k"], "q": self.tiles["k"] + self.tiles["v"]}
        self.early_rows = self.early["q"] + self.tiles["q"]


def loop(n, fn, unroll):
    trips = n // unroll

    def trip(g, carry):
        for u in range(unroll):
            fn(g * unroll + u)
        return carry

    if trips:
        lax.fori_loop(0, trips, trip, 0)
    for t in range(trips * unroll, n):
        fn(t)


def rows_at(t):
    return t * LANES if isinstance(t, int) else pl.multiple_of(t * LANES, LANES)


def column_sums(square):
    folded = square[:, :LANES]
    for at in range(LANES, square.shape[1], LANES):
        folded = folded + square[:, at : at + LANES]
    return jnp.sum(folded.T, axis=0, keepdims=True)


def kernel(plan, *refs):
    cols_n, rows_n = plan.cols_n, plan.rows_n
    width, rank = plan.width, plan.rank
    it = iter(refs)
    base = {p: None for p in NAMES}
    down, up, mag = dict(base), dict(base), dict(base)
    for p in NAMES:
        base[p], down[p], up[p], mag[p] = next(it), next(it), next(it), next(it)
    out = {p: next(it) for p in NAMES}
    stage, downs, ups, mags = {}, {}, {}, {}
    for p in NAMES:
        stage[p], downs[p], ups[p], mags[p] = next(it), next(it), next(it), next(it)
    wide = {p: next(it) for p in NAMES}
    send = {p: next(it) for p in NAMES}
    scale = next(it)
    spare = next(it)
    sums_early = next(it)
    parts = {p: next(it) for p in LATE}
    owned = {p: next(it) for p in LATE}
    totals = {p: next(it) for p in LATE}
    early_total = next(it)
    load_sem, own_sem, send_sem, recv_sem = (next(it) for _ in range(4))

    me = lax.axis_index("col")
    my_row = lax.axis_index("row")

    order = ("k", "v", "q", "o", "gate", "lift")
    loads = {}
    for i, p in enumerate(order):
        loads[p] = [
            pltpu.make_async_copy(src[p], dst[p], load_sem.at[4 * i + j])
            for j, (src, dst) in enumerate(((base, stage), (down, downs), (up, ups), (mag, mags)))
        ]

    def fetch(*names):
        for p in names:
            for copy in loads[p]:
                copy.start()

    fetch("k", "v", "q")

    barrier = pltpu.get_barrier_semaphore()
    for s in range(1, cols_n):
        pl.semaphore_signal(
            barrier, inc=1, device_id={"col": lax.rem(me + s, cols_n)}, device_id_type=MESH
        )
    for s in range(1, rows_n):
        pl.semaphore_signal(
            barrier, inc=1, device_id={"row": lax.rem(my_row + s, rows_n)}, device_id_type=MESH
        )

    def col_copy(kind, s, src, dst):
        return pltpu.make_async_remote_copy(
            src_ref=src,
            dst_ref=dst,
            send_sem=send_sem.at[kind, s],
            recv_sem=recv_sem.at[kind, s],
            device_id={"col": lax.rem(me + s, cols_n)},
            device_id_type=MESH,
        )

    def each(fn):
        def step(s, carry):
            fn(s)
            return carry

        lax.fori_loop(1, cols_n, step, 0)

    def direction(p, at, size):
        return stage[p][pl.ds(at, size), :].astype(jnp.float32) + lax.dot_general(
            ups[p][:, pl.ds(at, size)],
            downs[p][...],
            (((0,), (0,)), ((), ())),
            preferred_element_type=jnp.float32,
        )

    def first_pass(p, put, start, stop):
        height = plan.height[p]
        full = height // LANES

        def tile(t):
            at = rows_at(t)
            d = direction(p, at, LANES)
            wide[p][pl.ds(at, LANES), :] = d
            put(t, column_sums(d * d))

        loop(min(stop, full) - start, lambda t: tile(t + start), UNROLL)
        if stop > full:
            rest = height - full * LANES
            at = full * LANES
            d = direction(p, at, rest)
            wide[p][pl.ds(at, rest), :] = d
            fill = jnp.zeros((LANES - rest, width), jnp.float32)
            wide[p][pl.ds(at + rest, LANES - rest), :] = fill
            square = jnp.concatenate([d * d, fill], axis=0)
            put(full, column_sums(square))

    def magnitudes(p, t):
        full = plan.height[p] // LANES
        if isinstance(t, int) and t == full:
            rest = plan.height[p] - full * LANES
            spare[...] = jnp.zeros_like(spare)
            spare[0:1, 0:rest] = mags[p][full * LANES :].reshape(1, rest)
            return spare[0:1, :]
        return mags[p][pl.ds(rows_at(t), LANES)].reshape(1, LANES)

    def factors(p, t, total):
        return magnitudes(p, t) * lax.rsqrt(total + eps)

    def fill_scale(p, total_of):
        def one(t):
            row = factors(p, t, total_of(t))
            scale[pl.ds(rows_at(t), LANES), :] = jnp.broadcast_to(row, (LANES, LANES)).T

        full = plan.height[p] // LANES
        loop(full, one, UNROLL)
        if plan.tiles[p] > full:
            one(full)

    def merged(p, at, size):
        factor = scale[pl.ds(at, size), :]
        return jnp.concatenate(
            [
                (wide[p][pl.ds(at, size), c : c + LANES] * factor).astype(jnp.bfloat16)
                for c in range(0, width, LANES)
            ],
            axis=1,
        )

    KIND = {p: i for i, p in enumerate(ROW_SPLIT)}
    EARLY, O = len(ROW_SPLIT), len(ROW_SPLIT) + 1
    RS = {group: O + 1 + i for i, group in enumerate(LATE)}
    AG = {group: O + 3 + i for i, group in enumerate(LATE)}

    def block_copy(p, s):
        target = lax.rem(me + s, cols_n)
        return col_copy(
            KIND[p],
            s,
            send[p].at[target],
            out[p].at[:, pl.ds(pl.multiple_of(me * width, width), width)],
        )

    own = []

    def own_block(p, src, dst):
        copy = pltpu.make_async_copy(src, dst, own_sem.at[NAMES.index(p)])
        copy.start()
        own.append(copy)

    def own_rows(p):
        own_block(
            p, send[p].at[me], out[p].at[:, pl.ds(pl.multiple_of(me * width, width), width)]
        )

    def added(buffer):
        total = buffer[0]
        for c in range(1, cols_n):
            total = total + buffer[c]
        return total

    def arrive(p):
        for copy in loads[p]:
            copy.wait()

    def early_copy(s):
        return col_copy(EARLY, s, sums_early.at[me], sums_early.at[me])

    def put_early(p):
        def put(t, sums):
            sums_early[pl.ds(me, 1), pl.ds(plan.early[p] + t, 1), :] = sums.reshape(1, 1, LANES)

        return put

    for p in ("k", "v", "q"):
        arrive(p)
    fetch("gate", "o", "lift")
    for p in ("k", "v", "q"):
        first_pass(p, put_early(p), 0, plan.tiles[p])
    pl.semaphore_wait(barrier, cols_n + rows_n - 2)
    each(lambda s: early_copy(s).start())

    def place(p, t):
        group, begin = plan.begin[p]
        share = plan.share[group]
        return group, (begin + t) // share, (begin + t) % share

    def put_late(p):
        def put(t, sums):
            group, owner, at = place(p, t)
            parts[group][pl.ds(owner, 1), pl.ds(at, 1), :] = sums.reshape(1, 1, LANES)

        return put

    def late_total(p):
        def of(t):
            group, owner, at = place(p, t)
            return totals[group][pl.ds(owner, 1), pl.ds(at, 1), :].reshape(1, LANES)

        return of

    def rs_copy(group, s):
        target = lax.rem(me + s, cols_n)
        return col_copy(RS[group], s, parts[group].at[target], owned[group].at[me])

    def ag_copy(group, s):
        return col_copy(AG[group], s, totals[group].at[me], totals[group].at[me])

    def scatter(group):
        each(lambda s: rs_copy(group, s).start())
        owned[group][me] = parts[group][me]

    def gather(group):
        each(lambda s: rs_copy(group, s).wait_recv())
        totals[group][me] = added(owned[group])
        each(lambda s: ag_copy(group, s).start())

    def told(group):
        each(lambda s: ag_copy(group, s).wait_recv())

    def o_first(t):
        at = rows_at(t)
        d = direction("o", at, LANES).T
        wide["o"][:, pl.ds(at, LANES)] = d
        put_late("o")(t, jnp.sum(d * d, axis=0, keepdims=True))

    for group in LATE:
        parts[group][...] = jnp.zeros_like(parts[group])
    arrive("gate")
    first_pass("gate", put_late("gate"), 0, plan.tiles["gate"])
    arrive("o")
    loop(plan.tiles["o"], o_first, UNROLL)
    scatter("first")
    arrive("lift")
    first_pass("lift", put_late("lift"), 0, plan.tiles["lift"])
    scatter("second")

    each(lambda s: early_copy(s).wait_recv())
    early_total[...] = added(sums_early)

    def early_out(p):
        fill_scale(p, lambda t: early_total[pl.ds(plan.early[p] + t, 1), :])
        block = plan.block[p]

        def cut(c):
            at = c * block if isinstance(c, int) else pl.multiple_of(c * block, block)
            send[p][c] = merged(p, at, block)

        loop(cols_n, cut, UNROLL)
        each(lambda s: block_copy(p, s).start())
        own_rows(p)

    early_out("k")
    early_out("v")
    gather("first")
    early_out("q")
    gather("second")

    def make(p, target):
        block, held = plan.block[p], plan.held[p]
        window = up_to(block + 15, LANES)
        start = target * block
        at = pl.multiple_of(start // 16 * 16, 16)
        ahead = lax.broadcasted_iota(jnp.int32, (held, window), 1) - lax.broadcasted_iota(
            jnp.int32, (held, window), 0
        )
        pick = jnp.where(ahead == start - at, 1.0, 0.0).astype(jnp.bfloat16)
        rows = merged(p, at, window)
        send[p][target] = jnp.dot(pick, rows, preferred_element_type=jnp.float32).astype(
            jnp.bfloat16
        )

    def shifted_out(p):
        fill_scale(p, late_total(p))

        def one(s):
            make(p, lax.rem(me + s, cols_n))
            block_copy(p, s).start()

        each(one)
        make(p, me)
        own_rows(p)

    told("first")
    shifted_out("gate")

    def o_tile(t):
        at = rows_at(t)
        factor = factors("o", t, late_total("o")(t))
        send["o"][:, pl.ds(at, LANES)] = (wide["o"][:, pl.ds(at, LANES)] * factor).astype(
            jnp.bfloat16
        )

    loop(plan.tiles["o"], o_tile, UNROLL)
    depth = width // rows_n
    height = plan.height["o"]
    o_place = out["o"].at[:, pl.ds(pl.multiple_of(my_row * height, height), height)]

    def o_part(target):
        return send["o"].at[pl.ds(pl.multiple_of(target * depth, depth), depth), :]

    def o_copy(s):
        target = lax.rem(my_row + s, rows_n)
        return pltpu.make_async_remote_copy(
            src_ref=o_part(target),
            dst_ref=o_place,
            send_sem=send_sem.at[O, s],
            recv_sem=recv_sem.at[O, s],
            device_id={"row": target},
            device_id_type=MESH,
        )

    for s in range(1, rows_n):
        o_copy(s).start()
    own_block("o", o_part(my_row), o_place)

    told("second")
    shifted_out("lift")

    each(lambda s: early_copy(s).wait_send())
    for group in LATE:
        each(lambda s, group=group: rs_copy(group, s).wait_send())
        each(lambda s, group=group: ag_copy(group, s).wait_send())
    for copy in own:
        copy.wait()
    for s in range(1, rows_n):
        o_copy(s).wait()
    for p in ROW_SPLIT:
        each(lambda s, p=p: block_copy(p, s).wait())


def write_out(*refs):
    n = len(NAMES)
    copies = [pltpu.make_async_copy(refs[i], refs[n + i], refs[2 * n].at[i]) for i in range(n)]
    for copy in copies:
        copy.start()
    for copy in copies:
        copy.wait()


def solution(mesh):
    def on_device(*args):
        bases = {p: args[4 * i] for i, p in enumerate(NAMES)}
        rank = args[1].shape[0]
        plan = Plan(mesh, bases, rank)
        width, cols_n = plan.width, plan.cols_n
        bf16, f32 = jnp.bfloat16, jnp.float32
        operands, scratch = [], []
        for i, p in enumerate(NAMES):
            base, down, up, magnitude = args[4 * i : 4 * i + 4]
            operands += [base, down, up.T, magnitude]
            scratch += [
                pltpu.VMEM(base.shape, bf16),
                pltpu.VMEM(down.shape, bf16),
                pltpu.VMEM((rank, base.shape[0]), bf16),
                pltpu.VMEM(magnitude.shape, f32),
            ]
        shapes = []
        for p in NAMES:
            if p == "o":
                shapes.append((width // plan.rows_n, plan.height[p] * plan.rows_n))
                scratch.append(pltpu.VMEM((width, plan.height[p]), f32))
            else:
                shapes.append((plan.held[p], width * cols_n))
                scratch.append(pltpu.VMEM((plan.tiles[p] * LANES, width), f32))
        for p in NAMES:
            if p == "o":
                scratch.append(pltpu.VMEM((width, plan.height[p]), bf16))
            else:
                scratch.append(pltpu.VMEM((cols_n, plan.held[p], width), bf16))
        scratch.append(pltpu.VMEM((max(plan.tiles.values()) * LANES, LANES), f32))
        scratch.append(pltpu.VMEM((8, LANES), f32))
        scratch.append(pltpu.VMEM((cols_n, plan.early_rows, LANES), f32))
        scratch += [pltpu.VMEM((cols_n, plan.share[g], LANES), f32) for g in LATE] * 3
        scratch.append(pltpu.VMEM((plan.early_rows, LANES), f32))
        scratch += [
            pltpu.SemaphoreType.DMA((24,)),
            pltpu.SemaphoreType.DMA((6,)),
            pltpu.SemaphoreType.DMA((12, cols_n)),
            pltpu.SemaphoreType.DMA((12, cols_n)),
        ]
        got = pl.pallas_call(
            lambda *refs: kernel(plan, *refs),
            out_shape=[pltpu.VMEM(s, bf16) for s in shapes],
            in_specs=[pl.BlockSpec(memory_space=pl.ANY)] * len(operands),
            out_specs=[pl.BlockSpec(memory_space=pl.ANY)] * len(shapes),
            scratch_shapes=scratch,
            name="merge",
            compiler_params=pltpu.CompilerParams(
                collective_id=0, has_side_effects=True, vmem_limit_bytes=50 * 1024 * 1024
            ),
        )(*operands)
        got = pl.pallas_call(
            write_out,
            out_shape=[jax.ShapeDtypeStruct(s, bf16) for s in shapes],
            in_specs=[pl.BlockSpec(memory_space=pl.ANY)] * len(shapes),
            out_specs=[pl.BlockSpec(memory_space=pl.ANY)] * len(shapes),
            scratch_shapes=[pltpu.SemaphoreType.DMA((len(shapes),))],
            name="write_out",
            compiler_params=pltpu.CompilerParams(vmem_limit_bytes=2 * 1024 * 1024),
        )(*got)
        outs = []
        for p, o in zip(NAMES, got):
            outs.append(o.T if p == "o" else o[: plan.block[p]])
        return tuple(outs)

    specs = []
    for p in NAMES:
        specs += [P("row", "col"), P(None, "col"), P("row", None), P("row")]
    by_row = P(("row", "col"), None)
    return jax.shard_map(
        on_device,
        mesh=mesh,
        in_specs=tuple(specs),
        out_specs=(by_row, by_row, by_row, P(None, ("col", "row")), by_row, by_row),
        check_vma=False,
    )
```
